32 devices in a mesh: shard: 8 (over y, x, core), width: 4 (over z).
Axes of the slice: x: 2, y: 2, z: 4, core: 2. Of those that a mesh axis runs over, the one named last changes fastest.
Arguments:
- w_query: bfloat16 [5120, 5120], P('shard', 'width'), may hold values from -0.125 to 0.125
- low_query: bfloat16 [5120, 32], P('shard'), may hold values from -0.078125 to 0.078125
- high_query: bfloat16 [32, 5120], P(None, 'width'), may hold values from -1 to 1
- w_key: bfloat16 [5120, 5120], P('shard', 'width'), may hold values from -0.125 to 0.125
- low_key: bfloat16 [5120, 32], P('shard'), may hold values from -0.078125 to 0.078125
- high_key: bfloat16 [32, 5120], P(None, 'width'), may hold values from -1 to 1
- w_value: bfloat16 [5120, 5120], P('shard', 'width'), may hold values from -0.125 to 0.125
- low_value: bfloat16 [5120, 32], P('shard'), may hold values from -0.078125 to 0.078125
- high_value: bfloat16 [32, 5120], P(None, 'width'), may hold values from -1 to 1
- norm_train: float32 [5120], P(('shard', 'width')), may hold values from 0.25 to 1.75
- norm_step: float32 [5120], P(('shard', 'width')), may hold values from -0.3 to 0.3
Outputs:
- ready_query: bfloat16 [5120, 5120], P(None, 'width')
- ready_key: bfloat16 [5120, 5120], P(None, 'width')
- ready_value: bfloat16 [5120, 5120], P(None, 'width')
- factor_query: float32 [5120], P('width')
- factor_key: float32 [5120], P('width')
- factor_value: float32 [5120], P('width')
- serve_norm: bfloat16 [5120], replicated
The draws below stay inside these ranges and needn't reach their ends.
All inputs are finite; a program needn't handle non-finite values. Where the reference program divides by a largest or mean magnitude, that divisor is 1e-20 or more.
Results may differ from the reference program's by a relative error of at most 0.001.
Values may be sent and summed in bfloat16 or wider, within the bound.
A program may use at most 128 MiB of HBM per device.

```python
import jax
import jax.numpy as jnp

D_MODEL = 5120
Q_DIM = 5120
KV_DIM = 5120
RANK = 32


def with_spikes(result, own_key, source, target, parts, factor):
    def block_of(dim):
        return (jnp.arange(result.shape[dim]) // (result.shape[dim] // parts)).reshape((-1,) + (1,) * (result.ndim - 1 - dim))

    one_side = jax.random.permutation(own_key, parts)[block_of(target)]
    other_side = (block_of(target) + parts // 2) % parts
    return jnp.where((block_of(source) == one_side) | (block_of(source) == other_side), factor * result, result)


def steps_of(stream_key, extent, split, least, high):
    def one(position, shards_of):
        steps = jax.random.uniform(jax.random.fold_in(jax.random.fold_in(stream_key, 6), position), (shards_of,), jnp.float32, least / len(split), high / len(split))
        return jnp.repeat(jnp.exp(steps), extent[position] // shards_of).reshape((-1,) + (1,) * (len(extent) - position - 1))

    factor_of = one(*split[0])
    for cut in split[1:]:
        factor_of = factor_of * one(*cut)
    return factor_of


def scatter_about(key, extent, spread, reach, shards=(), kind=jnp.bfloat16):
    entries = jax.random.normal(key, extent, jnp.float32) * spread
    if len(shards) > 0:
        entries = steps_of(key, extent, shards, -0.22, 0.18) * entries
    return jnp.clip(entries, min=-reach, max=reach).astype(kind)


def noise_with(key, extent, spread, most, cuts, heavy, kind=jnp.bfloat16):
    result = spread * jax.random.normal(key, extent, jnp.float32)
    if cuts:
        result = result * steps_of(key, extent, cuts, -0.22, 0.18)
    return jnp.clip(with_spikes(result, jax.random.fold_in(key, 3), *heavy), -most, most).astype(kind)


def setup_inputs(seed: int = 0) -> dict:
    splits = jax.random.split(jax.random.key(seed), 12)
    w_query = noise_with(splits[0], (D_MODEL, Q_DIM), D_MODEL ** -0.5, 0.125, ((0, 8), (1, 4)), (0, 1, 8, 2.0))
    low_query = scatter_about(splits[1], (D_MODEL, RANK), D_MODEL ** -0.5, 0.078125, ((0, 8),))
    high_query = scatter_about(splits[2], (RANK, Q_DIM), RANK ** -0.5, 1.0, ((1, 4),))
    w_key = noise_with(splits[3], (D_MODEL, KV_DIM), D_MODEL ** -0.5, 0.125, ((0, 8), (1, 4)), (0, 1, 8, 2.0))
    low_key = scatter_about(splits[4], (D_MODEL, RANK), D_MODEL ** -0.5, 0.078125, ((0, 8),))
    high_key = scatter_about(splits[5], (RANK, KV_DIM), RANK ** -0.5, 1.0, ((1, 4),))
    w_value = noise_with(splits[6], (D_MODEL, KV_DIM), D_MODEL ** -0.5, 0.125, ((0, 8), (1, 4)), (0, 1, 8, 2.0))
    low_value = scatter_about(splits[7], (D_MODEL, RANK), D_MODEL ** -0.5, 0.078125, ((0, 8),))
    high_value = scatter_about(splits[8], (RANK, KV_DIM), RANK ** -0.5, 1.0, ((1, 4),))
    norm_train = jnp.clip(1.0 + 0.15 * jax.random.normal(splits[9], (D_MODEL,), jnp.float32), 0.25, 1.75)
    norm_step = jnp.clip(jax.random.uniform(splits[10], (D_MODEL,), jnp.float32, -0.3, 0.3) * steps_of(splits[10], (D_MODEL,), ((0, 32),), -0.4, 0.0), -0.3, 0.3)
    return dict(w_query=w_query, low_query=low_query, high_query=high_query, w_key=w_key, low_key=low_key, high_key=high_key, w_value=w_value, low_value=low_value, high_value=high_value, norm_train=norm_train, norm_step=norm_step)


mix_rate = 0.5


def reference(w_query, low_query, high_query, w_key, low_key, high_key, w_value, low_value, high_value, norm_train, norm_step):
    latest_query = w_query.astype(jnp.float32) + mix_rate * jnp.dot(low_query, high_query, preferred_element_type=jnp.float32)
    latest_key = w_key.astype(jnp.float32) + mix_rate * jnp.dot(low_key, high_key, preferred_element_type=jnp.float32)
    latest_value = w_value.astype(jnp.float32) + mix_rate * jnp.dot(low_value, high_value, preferred_element_type=jnp.float32)
    factor_query = jnp.max(jnp.abs(latest_query), axis=0)
    ready_query = (latest_query / factor_query).astype(jnp.bfloat16)
    factor_key = jnp.max(jnp.abs(latest_key), axis=0)
    ready_key = (latest_key / factor_key).astype(jnp.bfloat16)
    factor_value = jnp.max(jnp.abs(latest_value), axis=0)
    ready_value = (latest_value / factor_value).astype(jnp.bfloat16)
    serve_norm = (norm_train + norm_step).astype(jnp.bfloat16)
    return ready_query, ready_key, ready_value, factor_query, factor_key, factor_value, serve_norm
```

```python
import functools

import jax
import jax.numpy as jnp
from jax import lax
from jax.experimental import pallas as pl
from jax.experimental.pallas import tpu as pltpu
from jax.sharding import PartitionSpec as P

mix_rate = 0.5
MESH = pl.DeviceIdType.MESH
ANY = pl.BlockSpec(memory_space=pl.ANY)


def chunks_of(rows):
    for count in (5, 4, 2):
        if rows % (2 * count * 16) == 0:
            return count
    return 1


def gather_kernel(n, width, *refs):
    weights, lows, highs, norms = refs[0:3], refs[3:6], refs[6:9], refs[9:11]
    ready, factors, gains = refs[11], refs[12:15], refs[15]
    w_mem, low_mem, high_mem, norm_mem, latest, scale, maxima = refs[16:23]
    load_sem, send_sem, max_send, max_recv, norm_send, norm_recv = refs[23:29]
    ring_sem, pair_sem, low_turned = refs[29:32]
    outs = [ready.at[m] for m in range(3)]

    rows = w_mem.shape[1]
    chips = n // 2
    half = chips // 2
    count = chunks_of(rows)
    piece = rows // (2 * count)
    steps = 3 * count

    me = lax.axis_index("shard")
    line = lax.axis_index("width")
    chip, core = me // 2, lax.rem(me, 2)
    sibling = me + 1 - 2 * core

    def turned(c):
        return jnp.where(c < half, c, chips + half - 1 - c)

    place = turned(chip)

    def shard_at(offset):
        return turned(lax.rem(place + offset + 2 * chips, chips)) * 2 + core

    loads = []
    for m in range(3):
        group = []
        for source, target in (
            (weights[m], w_mem.at[m]),
            (lows[m], low_turned.at[m]),
            (highs[m], high_mem.at[m]),
        ):
            group.append(pltpu.make_async_copy(source, target, load_sem.at[m, len(group)]))
        loads.append(group)
    norm_loads = [
        pltpu.make_async_copy(norms[i], norm_mem.at[i], load_sem.at[3, i]) for i in range(2)
    ]
    for group in loads:
        for copy in group:
            copy.start()
    for copy in norm_loads:
        copy.start()

    barrier = pltpu.get_barrier_semaphore()
    for step in range(1, n):
        pl.semaphore_signal(
            barrier, inc=1, device_id={"shard": lax.rem(me + step, n)}, device_id_type=MESH
        )
    for step in range(1, width):
        pl.semaphore_signal(
            barrier, inc=1, device_id={"width": lax.rem(line + step, width)}, device_id_type=MESH
        )

    tile = piece

    def merge(m):
        for copy in loads[m]:
            copy.wait()
        low_mem[m] = low_turned[m].T

        def body(t, largest):
            at = pl.ds(pl.multiple_of(t * tile, tile), tile)
            value = w_mem[m, at, :].astype(jnp.float32) + mix_rate * jnp.dot(
                low_mem[m, at, :], high_mem[m], preferred_element_type=jnp.float32
            )
            latest[m, at, :] = value
            return jnp.maximum(largest, jnp.max(jnp.abs(value), axis=0, keepdims=True))

        largest = lax.fori_loop(0, rows // tile, body, jnp.zeros((1, w_mem.shape[2]), jnp.float32))
        maxima[m, me] = largest

    def share(m):
        for step in range(1, n):
            pltpu.make_async_remote_copy(
                src_ref=maxima.at[m, me],
                dst_ref=maxima.at[m, me],
                send_sem=max_send.at[m],
                recv_sem=max_recv.at[m],
                device_id={"shard": lax.rem(me + step, n)},
                device_id_type=MESH,
            ).start()

    def settle(m):
        others = maxima.at[m, pl.ds(0, n - 1)]
        pltpu.make_async_copy(others, others, max_recv.at[m]).wait()
        factor = jnp.max(maxima[m], axis=0)
        factors[m][...] = factor
        scale[m] = 1.0 / factor

    def rows_of(letter, k):
        return ((letter * count) + k % count) * piece

    def finish(k):
        m = k // count
        for letter in range(2):
            at = pl.ds(rows_of(letter, k), piece)
            ready[m, me, at, :] = (latest[m, at, :] * scale[m]).astype(jnp.bfloat16)

    def view(k, letter, owner):
        return outs[k // count].at[owner, pl.ds(rows_of(letter, k), piece)]

    def ring_copy(k, side, letter, hop):
        sign = 1 - 2 * side
        owner = shard_at(-sign * hop)
        where = view(k, letter, owner)
        return pltpu.make_async_remote_copy(
            src_ref=where,
            dst_ref=where,
            send_sem=send_sem.at[k // count],
            recv_sem=ring_sem.at[k, side, letter, hop],
            device_id={"shard": shard_at(sign)},
            device_id_type=MESH,
        )

    def ring_arrival(k, side, letter, hop):
        sign = 1 - 2 * side
        owner = shard_at(-sign * (hop + 1))
        where = view(k, letter, owner)
        pltpu.make_async_copy(where, where, ring_sem.at[k, side, letter, hop]).wait()
        return owner

    def pair_copy(k, letter, owner):
        where = view(k, letter, owner)
        pltpu.make_async_remote_copy(
            src_ref=where,
            dst_ref=where,
            send_sem=send_sem.at[k // count],
            recv_sem=pair_sem.at[k // count],
            device_id={"shard": sibling},
            device_id_type=MESH,
        ).start()

    def hops(side, letter):
        return half if side == letter else half - 1

    merge(0)
    pl.semaphore_wait(barrier, n - 1 + width - 1)
    share(0)
    for copy in norm_loads:
        copy.wait()
    gains[me, line] = norm_mem[0] + norm_mem[1]
    for step in range(1, width):
        pltpu.make_async_remote_copy(
            src_ref=gains.at[me, line],
            dst_ref=gains.at[me, line],
            send_sem=norm_send.at[0],
            recv_sem=norm_recv.at[0],
            device_id={"width": lax.rem(line + step, width)},
            device_id_type=MESH,
        ).start()
    merge(1)
    share(1)
    settle(0)
    finish(0)

    for j in range(steps + half + 1):
        if j < steps:
            for side in range(2):
                if hops(side, side) > 0:
                    ring_copy(j, side, side, 0).start()
        for hop in range(half):
            k = j - 1 - hop
            if 0 <= k < steps and hop + 1 < half:
                for side in range(2):
                    owner = ring_arrival(k, side, side, hop)
                    ring_copy(k, side, side, hop + 1).start()
                    pair_copy(k, side, owner)
        if j < steps:
            for side in range(2):
                if hops(side, 1 - side) > 0:
                    ring_copy(j, side, 1 - side, 0).start()
        for hop in range(half - 1):
            k = j - 1 - hop
            if 0 <= k < steps and hop + 1 < half - 1:
                for side in range(2):
                    owner = ring_arrival(k, side, 1 - side, hop)
                    ring_copy(k, side, 1 - side, hop + 1).start()
                    pair_copy(k, 1 - side, owner)
        if j < steps:
            for letter in range(2):
                pair_copy(j, letter, me)
        if j == 0:
            merge(2)
            share(2)
            ours = gains.at[me, pl.ds(0, width - 1)]
            if width > 1:
                pltpu.make_async_copy(ours, ours, norm_recv.at[0]).wait()
            for step in range(1, n):
                pltpu.make_async_remote_copy(
                    src_ref=gains.at[me],
                    dst_ref=gains.at[me],
                    send_sem=norm_send.at[1],
                    recv_sem=norm_recv.at[1],
                    device_id={"shard": lax.rem(me + step, n)},
                    device_id_type=MESH,
                ).start()
        if j + 1 < steps:
            if (j + 1) % count == 0:
                settle((j + 1) // count)
            finish(j + 1)
        for side in range(2):
            for letter in (side, 1 - side):
                hop = hops(side, letter) - 1
                k = j - 2 - hop
                if hop >= 0 and 0 <= k < steps:
                    owner = ring_arrival(k, side, letter, hop)
                    pair_copy(k, letter, owner)

    for m in range(3):
        theirs = outs[m].at[pl.ds(0, chips)]
        pltpu.make_async_copy(theirs, theirs, pair_sem.at[m]).wait()
        sent = outs[m].at[pl.ds(0, n - 1)]
        pltpu.make_async_copy(sent, sent, send_sem.at[m]).wait()
        others = maxima.at[m, pl.ds(0, n - 1)]
        pltpu.make_async_copy(others, others, max_send.at[m]).wait()
    ours = gains.at[me, pl.ds(0, width - 1)]
    pltpu.make_async_copy(ours, ours, norm_send.at[0]).wait()
    block = gains.at[pl.ds(0, n - 1)]
    pltpu.make_async_copy(block, block, norm_recv.at[1]).wait()
    pltpu.make_async_copy(block, block, norm_send.at[1]).wait()


def place_kernel(*refs):
    source, targets, sem = refs[0], refs[1:4], refs[4]
    copies = []
    for m in range(3):
        for i in range(source.shape[1]):
            copies.append(
                pltpu.make_async_copy(source.at[m, i], targets[m].at[i], sem.at[m, i])
            )
    for copy in copies:
        copy.start()
    for copy in copies:
        copy.wait()


def body(n, width, w_query, low_query, high_query, w_key, low_key, high_key, w_value, low_value, high_value, norm_train, norm_step):
    rows, columns = w_query.shape
    rank = low_query.shape[1]
    length = norm_train.shape[0]
    half = n // 4
    steps = 3 * chunks_of(rows)
    results = pl.pallas_call(
        functools.partial(gather_kernel, n, width),
        name="merge_gather",
        out_shape=[pltpu.VMEM((3, n, rows, columns), jnp.bfloat16)]
        + [jax.ShapeDtypeStruct((1, columns), jnp.float32)] * 3
        + [jax.ShapeDtypeStruct((n, width, 1, length), jnp.float32)],
        in_specs=[ANY] * 11,
        out_specs=[pl.BlockSpec(memory_space=pltpu.VMEM)] * 5,
        scratch_shapes=[
            pltpu.VMEM((3, rows, columns), jnp.bfloat16),
            pltpu.VMEM((3, rows, rank), jnp.bfloat16),
            pltpu.VMEM((3, rank, columns), jnp.bfloat16),
            pltpu.VMEM((2, 1, length), jnp.float32),
            pltpu.VMEM((3, rows, columns), jnp.float32),
            pltpu.VMEM((3, 1, columns), jnp.float32),
            pltpu.VMEM((3, n, 1, columns), jnp.float32),
            pltpu.SemaphoreType.DMA((4, 3)),
            pltpu.SemaphoreType.DMA((3,)),
            pltpu.SemaphoreType.DMA((3,)),
            pltpu.SemaphoreType.DMA((3,)),
            pltpu.SemaphoreType.DMA((2,)),
            pltpu.SemaphoreType.DMA((2,)),
            pltpu.SemaphoreType.DMA((steps, 2, 2, half)),
            pltpu.SemaphoreType.DMA((3,)),
            pltpu.VMEM((3, rank, rows), jnp.bfloat16),
        ],
        compiler_params=pltpu.CompilerParams(
            collective_id=0, has_side_effects=True, vmem_limit_bytes=20 * 2**20
        ),
    )(
        w_query, w_key, w_value,
        low_query.T, low_key.T, low_value.T,
        high_query, high_key, high_value,
        norm_train.reshape(1, length), norm_step.reshape(1, length),
    )
    readies = pl.pallas_call(
        place_kernel,
        name="place",
        out_shape=[jax.ShapeDtypeStruct((n, rows, columns), jnp.bfloat16)] * 3,
        in_specs=[ANY],
        out_specs=[ANY] * 3,
        scratch_shapes=[pltpu.SemaphoreType.DMA((3, n))],
        compiler_params=pltpu.CompilerParams(vmem_limit_bytes=2**20),
    )(pltpu.with_memory_space_constraint(results[0], pltpu.VMEM))
    return (
        *(ready.reshape(n * rows, columns) for ready in readies),
        *(factor.reshape(columns) for factor in results[1:4]),
        results[4].astype(jnp.bfloat16).reshape(n * width * length),
    )


def solution(mesh):
    n, width = mesh.shape["shard"], mesh.shape["width"]
    return jax.shard_map(
        functools.partial(body, n, width),
        mesh=mesh,
        in_specs=(
            P("shard", "width"),
            P("shard", None),
            P(None, "width"),
            P("shard", "width"),
            P("shard", None),
            P(None, "width"),
            P("shard", "width"),
            P("shard", None),
            P(None, "width"),
            P(("shard", "width")),
            P(("shard", "width")),
        ),
        out_specs=(
            P(None, "width"),
            P(None, "width"),
            P(None, "width"),
            P("width"),
            P("width"),
            P("width"),
            P(),
        ),
        check_vma=False,
    )
```

```python
import functools

import jax
import jax.numpy as jnp
from jax import lax
from jax.experimental import pallas as pl
from jax.experimental.pallas import tpu as pltpu
from jax.sharding import PartitionSpec as P

mix_rate = 0.5
MESH = pl.DeviceIdType.MESH
ANY = pl.BlockSpec(memory_space=pl.ANY)


def chunks_of(rows):
    for count in (5, 4, 2):
        if rows % (2 * count * 16) == 0:
            return count
    return 1


def gather_kernel(n, width, *refs):
    weights, lows, highs, norms = refs[0:3], refs[3:6], refs[6:9], refs[9:11]
    ready, factors, gains = refs[11], refs[12:15], refs[15]
    w_mem, low_mem, high_mem, norm_mem, latest, scale, maxima = refs[16:23]
    load_sem, send_sem, max_send, max_recv, norm_send, norm_recv = refs[23:29]
    ring_sem, pair_sem, low_turned = refs[29:32]
    outs = [ready.at[m] for m in range(3)]

    rows = w_mem.shape[1]
    chips = n // 2
    half = chips // 2
    count = chunks_of(rows)
    piece = rows // (2 * count)
    steps = 3 * count

    me = lax.axis_index("shard")
    line = lax.axis_index("width")
    chip, core = me // 2, lax.rem(me, 2)
    sibling = me + 1 - 2 * core

    def turned(c):
        return jnp.where(c < half, c, chips + half - 1 - c)

    place = turned(chip)

    def shard_at(offset):
        return turned(lax.rem(place + offset + 2 * chips, chips)) * 2 + core

    loads = []
    for m in range(3):
        group = []
        for source, target in (
            (weights[m], w_mem.at[m]),
            (lows[m], low_turned.at[m]),
            (highs[m], high_mem.at[m]),
        ):
            group.append(pltpu.make_async_copy(source, target, load_sem.at[m, len(group)]))
        loads.append(group)
    norm_loads = [
        pltpu.make_async_copy(norms[i], norm_mem.at[i], load_sem.at[3, i]) for i in range(2)
    ]
    for group in loads:
        for copy in group:
            copy.start()
    for copy in norm_loads:
        copy.start()

    barrier = pltpu.get_barrier_semaphore()
    for step in range(1, n):
        pl.semaphore_signal(
            barrier, inc=1, device_id={"shard": lax.rem(me + step, n)}, device_id_type=MESH
        )
    for step in range(1, width):
        pl.semaphore_signal(
            barrier, inc=1, device_id={"width": lax.rem(line + step, width)}, device_id_type=MESH
        )

    tile = piece

    def merge(m):
        for copy in loads[m]:
            copy.wait()
        low_mem[m] = low_turned[m].T

        def body(t, largest):
            at = pl.ds(pl.multiple_of(t * tile, tile), tile)
            value = w_mem[m, at, :].astype(jnp.float32) + mix_rate * jnp.dot(
                low_mem[m, at, :], high_mem[m], preferred_element_type=jnp.float32
            )
            latest[m, at, :] = value
            sizes = jnp.abs(value).reshape(tile // 8, 8, value.shape[1])
            return jnp.maximum(largest, jnp.max(sizes, axis=0))

        largest = lax.fori_loop(0, rows // tile, body, jnp.zeros((8, w_mem.shape[2]), jnp.float32))
        maxima[m, me] = jnp.max(largest, axis=0, keepdims=True)

    def share(m):
        for step in range(1, n):
            pltpu.make_async_remote_copy(
                src_ref=maxima.at[m, me],
                dst_ref=maxima.at[m, me],
                send_sem=max_send.at[m],
                recv_sem=max_recv.at[m],
                device_id={"shard": lax.rem(me + step, n)},
                device_id_type=MESH,
            ).start()

    def settle(m):
        others = maxima.at[m, pl.ds(0, n - 1)]
        pltpu.make_async_copy(others, others, max_recv.at[m]).wait()
        factor = jnp.max(maxima[m], axis=0)
        factors[m][...] = factor
        scale[m] = 1.0 / factor

    def rows_of(letter, k):
        return ((letter * count) + k % count) * piece

    def finish(k):
        m = k // count
        for letter in range(2):
            at = pl.ds(rows_of(letter, k), piece)
            ready[m, me, at, :] = (latest[m, at, :] * scale[m]).astype(jnp.bfloat16)

    def view(k, letter, owner):
        return outs[k // count].at[owner, pl.ds(rows_of(letter, k), piece)]

    def ring_copy(k, side, letter, hop):
        sign = 1 - 2 * side
        owner = shard_at(-sign * hop)
        where = view(k, letter, owner)
        return pltpu.make_async_remote_copy(
            src_ref=where,
            dst_ref=where,
            send_sem=send_sem.at[k // count],
            recv_sem=ring_sem.at[k, side, letter, hop],
            device_id={"shard": shard_at(sign)},
            device_id_type=MESH,
        )

    def ring_arrival(k, side, letter, hop):
        sign = 1 - 2 * side
        owner = shard_at(-sign * (hop + 1))
        where = view(k, letter, owner)
        pltpu.make_async_copy(where, where, ring_sem.at[k, side, letter, hop]).wait()
        return owner

    def pair_copy(k, letter, owner):
        where = view(k, letter, owner)
        pltpu.make_async_remote_copy(
            src_ref=where,
            dst_ref=where,
            send_sem=send_sem.at[k // count],
            recv_sem=pair_sem.at[k // count],
            device_id={"shard": sibling},
            device_id_type=MESH,
        ).start()

    def hops(side, letter):
        return half if side == letter else half - 1

    merge(0)
    pl.semaphore_wait(barrier, n - 1 + width - 1)
    share(0)
    settle(0)
    finish(0)

    for j in range(steps + half + 1):
        if j < steps:
            for side in range(2):
                if hops(side, side) > 0:
                    ring_copy(j, side, side, 0).start()
        for hop in range(half):
            k = j - 1 - hop
            if 0 <= k < steps and hop + 1 < half:
                for side in range(2):
                    owner = ring_arrival(k, side, side, hop)
                    ring_copy(k, side, side, hop + 1).start()
                    pair_copy(k, side, owner)
        if j < steps:
            for side in range(2):
                if hops(side, 1 - side) > 0:
                    ring_copy(j, side, 1 - side, 0).start()
        for hop in range(half - 1):
            k = j - 1 - hop
            if 0 <= k < steps and hop + 1 < half - 1:
                for side in range(2):
                    owner = ring_arrival(k, side, 1 - side, hop)
                    ring_copy(k, side, 1 - side, hop + 1).start()
                    pair_copy(k, 1 - side, owner)
        if j < steps:
            for letter in range(2):
                pair_copy(j, letter, me)
        if j == 0:
            merge(1)
            share(1)
            for copy in norm_loads:
                copy.wait()
            gains[me, line] = norm_mem[0] + norm_mem[1]
            for step in range(1, width):
                pltpu.make_async_remote_copy(
                    src_ref=gains.at[me, line],
                    dst_ref=gains.at[me, line],
                    send_sem=norm_send.at[0],
                    recv_sem=norm_recv.at[0],
                    device_id={"width": lax.rem(line + step, width)},
                    device_id_type=MESH,
                ).start()
        if j == 1:
            merge(2)
            share(2)
            ours = gains.at[me, pl.ds(0, width - 1)]
            if width > 1:
                pltpu.make_async_copy(ours, ours, norm_recv.at[0]).wait()
            for step in range(1, n):
                pltpu.make_async_remote_copy(
                    src_ref=gains.at[me],
                    dst_ref=gains.at[me],
                    send_sem=norm_send.at[1],
                    recv_sem=norm_recv.at[1],
                    device_id={"shard": lax.rem(me + step, n)},
                    device_id_type=MESH,
                ).start()
        if j + 1 < steps:
            if (j + 1) % count == 0:
                settle((j + 1) // count)
            finish(j + 1)
        for side in range(2):
            for letter in (side, 1 - side):
                hop = hops(side, letter) - 1
                k = j - 2 - hop
                if hop >= 0 and 0 <= k < steps:
                    owner = ring_arrival(k, side, letter, hop)
                    pair_copy(k, letter, owner)

    for m in range(3):
        theirs = outs[m].at[pl.ds(0, chips)]
        pltpu.make_async_copy(theirs, theirs, pair_sem.at[m]).wait()
        sent = outs[m].at[pl.ds(0, n - 1)]
        pltpu.make_async_copy(sent, sent, send_sem.at[m]).wait()
        others = maxima.at[m, pl.ds(0, n - 1)]
        pltpu.make_async_copy(others, others, max_send.at[m]).wait()
    ours = gains.at[me, pl.ds(0, width - 1)]
    pltpu.make_async_copy(ours, ours, norm_send.at[0]).wait()
    block = gains.at[pl.ds(0, n - 1)]
    pltpu.make_async_copy(block, block, norm_recv.at[1]).wait()
    pltpu.make_async_copy(block, block, norm_send.at[1]).wait()


def place_kernel(*refs):
    source, small = refs[0], refs[1:5]
    targets, scales, serve, sem = refs[5:8], refs[8:11], refs[11], refs[12]
    factors, gains, small_sem = refs[13:16], refs[16], refs[17]
    loads = [
        pltpu.make_async_copy(small[i], refs[13 + i], small_sem.at[i]) for i in range(4)
    ]
    for copy in loads:
        copy.start()
    copies = []
    for m in range(3):
        for i in range(source.shape[1]):
            copies.append(
                pltpu.make_async_copy(source.at[m, i], targets[m].at[i], sem.at[m, i])
            )
    for copy in copies:
        copy.start()
    for copy in loads:
        copy.wait()
    for m in range(3):
        scales[m][...] = factors[m][...].reshape(scales[m].shape)
    blocks = [gains[i, k] for i in range(gains.shape[0]) for k in range(gains.shape[1])]
    line = jnp.concatenate(blocks, axis=1)
    serve[...] = line.reshape(serve.shape).astype(jnp.bfloat16)
    for copy in copies:
        copy.wait()


def body(n, width, w_query, low_query, high_query, w_key, low_key, high_key, w_value, low_value, high_value, norm_train, norm_step):
    rows, columns = w_query.shape
    rank = low_query.shape[1]
    length = norm_train.shape[0]
    half = n // 4
    steps = 3 * chunks_of(rows)
    results = pl.pallas_call(
        functools.partial(gather_kernel, n, width),
        name="merge_gather",
        out_shape=[pltpu.VMEM((3, n, rows, columns), jnp.bfloat16)]
        + [jax.ShapeDtypeStruct((1, columns), jnp.float32)] * 3
        + [jax.ShapeDtypeStruct((n, width, 1, length), jnp.float32)],
        in_specs=[ANY] * 11,
        out_specs=[pl.BlockSpec(memory_space=pltpu.VMEM)] * 5,
        scratch_shapes=[
            pltpu.VMEM((3, rows, columns), jnp.bfloat16),
            pltpu.VMEM((3, rows, rank), jnp.bfloat16),
            pltpu.VMEM((3, rank, columns), jnp.bfloat16),
            pltpu.VMEM((2, 1, length), jnp.float32),
            pltpu.VMEM((3, rows, columns), jnp.float32),
            pltpu.VMEM((3, 1, columns), jnp.float32),
            pltpu.VMEM((3, n, 1, columns), jnp.float32),
            pltpu.SemaphoreType.DMA((4, 3)),
            pltpu.SemaphoreType.DMA((3,)),
            pltpu.SemaphoreType.DMA((3,)),
            pltpu.SemaphoreType.DMA((3,)),
            pltpu.SemaphoreType.DMA((2,)),
            pltpu.SemaphoreType.DMA((2,)),
            pltpu.SemaphoreType.DMA((steps, 2, 2, half)),
            pltpu.SemaphoreType.DMA((3,)),
            pltpu.VMEM((3, rank, rows), jnp.bfloat16),
        ],
        compiler_params=pltpu.CompilerParams(
            collective_id=0, has_side_effects=True, vmem_limit_bytes=20 * 2**20
        ),
    )(
        w_query, w_key, w_value,
        low_query.T, low_key.T, low_value.T,
        high_query, high_key, high_value,
        norm_train.reshape(1, length), norm_step.reshape(1, length),
    )
    placed = pl.pallas_call(
        place_kernel,
        name="place",
        out_shape=[jax.ShapeDtypeStruct((n, rows, columns), jnp.bfloat16)] * 3
        + [jax.ShapeDtypeStruct((columns,), jnp.float32)] * 3
        + [jax.ShapeDtypeStruct((n * width * length,), jnp.bfloat16)],
        in_specs=[ANY] + [pl.BlockSpec(memory_space=pltpu.HBM)] * 4,
        out_specs=[ANY] * 3 + [pl.BlockSpec(memory_space=pltpu.VMEM)] * 4,
        scratch_shapes=[
            pltpu.SemaphoreType.DMA((3, n)),
            *[pltpu.VMEM((1, columns), jnp.float32)] * 3,
            pltpu.VMEM((n, width, 1, length), jnp.float32),
            pltpu.SemaphoreType.DMA((4,)),
        ],
        compiler_params=pltpu.CompilerParams(vmem_limit_bytes=2**20),
    )(pltpu.with_memory_space_constraint(results[0], pltpu.VMEM), *(pltpu.with_memory_space_constraint(small, pltpu.HBM) for small in results[1:]))
    return (
        *(ready.reshape(n * rows, columns) for ready in placed[0:3]),
        *placed[3:],
    )


def solution(mesh):
    n, width = mesh.shape["shard"], mesh.shape["width"]
    return jax.shard_map(
        functools.partial(body, n, width),
        mesh=mesh,
        in_specs=(
            P("shard", "width"),
            P("shard", None),
            P(None, "width"),
            P("shard", "width"),
            P("shard", None),
            P(None, "width"),
            P("shard", "width"),
            P("shard", None),
            P(None, "width"),
            P(("shard", "width")),
            P(("shard", "width")),
        ),
        out_specs=(
            P(None, "width"),
            P(None, "width"),
            P(None, "width"),
            P("width"),
            P("width"),
            P("width"),
            P(),
        ),
        check_vma=False,
    )
```

```python
import functools

import jax
import jax.numpy as jnp
from jax import lax
from jax.experimental import pallas as pl
from jax.experimental.pallas import tpu as pltpu
from jax.sharding import PartitionSpec as P

mix_rate = 0.5
MESH = pl.DeviceIdType.MESH
ANY = pl.BlockSpec(memory_space=pl.ANY)


def chunks_of(rows):
    for count in (5, 4, 2):
        if rows % (2 * count * 16) == 0:
            return count
    return 1


def gather_kernel(n, width, *refs):
    weights, lows, highs, norms = refs[0:3], refs[3:6], refs[6:9], refs[9:11]
    ready, small_outs = refs[11], refs[12:16]
    w_mem, low_mem, high_mem, norm_mem, latest, scale, maxima = refs[16:23]
    load_sem, send_sem, max_send, max_recv, norm_send, norm_recv = refs[23:29]
    ring_sem, pair_sem, low_turned, held, gains, out_sem = refs[29:35]
    outs = [ready.at[m] for m in range(3)]

    rows = w_mem.shape[1]
    chips = n // 2
    half = chips // 2
    count = chunks_of(rows)
    piece = rows // (2 * count)
    steps = 3 * count

    me = lax.axis_index("shard")
    line = lax.axis_index("width")
    chip, core = me // 2, lax.rem(me, 2)
    sibling = me + 1 - 2 * core

    def turned(c):
        return jnp.where(c < half, c, chips + half - 1 - c)

    place = turned(chip)

    def shard_at(offset):
        return turned(lax.rem(place + offset + 2 * chips, chips)) * 2 + core

    loads = []
    for m in range(3):
        group = []
        for source, target in (
            (weights[m], w_mem.at[m]),
            (lows[m], low_turned.at[m]),
            (highs[m], high_mem.at[m]),
        ):
            group.append(pltpu.make_async_copy(source, target, load_sem.at[m, len(group)]))
        loads.append(group)
    norm_loads = [
        pltpu.make_async_copy(norms[i], norm_mem.at[i], load_sem.at[3, i]) for i in range(2)
    ]
    for group in loads:
        for copy in group:
            copy.start()
    for copy in norm_loads:
        copy.start()

    barrier = pltpu.get_barrier_semaphore()
    for step in range(1, n):
        pl.semaphore_signal(
            barrier, inc=1, device_id={"shard": lax.rem(me + step, n)}, device_id_type=MESH
        )
    for step in range(1, width):
        pl.semaphore_signal(
            barrier, inc=1, device_id={"width": lax.rem(line + step, width)}, device_id_type=MESH
        )

    tile = piece

    def merge(m):
        for copy in loads[m]:
            copy.wait()
        low_mem[m] = low_turned[m].T

        def body(t, largest):
            at = pl.ds(pl.multiple_of(t * tile, tile), tile)
            value = w_mem[m, at, :].astype(jnp.float32) + mix_rate * jnp.dot(
                low_mem[m, at, :], high_mem[m], preferred_element_type=jnp.float32
            )
            latest[m, at, :] = value
            sizes = jnp.abs(value).reshape(tile // 8, 8, value.shape[1])
            return jnp.maximum(largest, jnp.max(sizes, axis=0))

        largest = lax.fori_loop(0, rows // tile, body, jnp.zeros((8, w_mem.shape[2]), jnp.float32))
        maxima[m, me] = jnp.max(largest, axis=0, keepdims=True)

    def share(m):
        for step in range(1, n):
            pltpu.make_async_remote_copy(
                src_ref=maxima.at[m, me],
                dst_ref=maxima.at[m, me],
                send_sem=max_send.at[m],
                recv_sem=max_recv.at[m],
                device_id={"shard": lax.rem(me + step, n)},
                device_id_type=MESH,
            ).start()

    def settle(m):
        others = maxima.at[m, pl.ds(0, n - 1)]
        pltpu.make_async_copy(others, others, max_recv.at[m]).wait()
        factor = jnp.max(maxima[m], axis=0)
        held[m] = factor
        scale[m] = 1.0 / factor

    def rows_of(letter, k):
        return ((letter * count) + k % count) * piece

    def finish(k):
        m = k // count
        for letter in range(2):
            at = pl.ds(rows_of(letter, k), piece)
            ready[m, me, at, :] = (latest[m, at, :] * scale[m]).astype(jnp.bfloat16)

    def view(k, letter, owner):
        return outs[k // count].at[owner, pl.ds(rows_of(letter, k), piece)]

    def ring_copy(k, side, letter, hop):
        sign = 1 - 2 * side
        owner = shard_at(-sign * hop)
        where = view(k, letter, owner)
        return pltpu.make_async_remote_copy(
            src_ref=where,
            dst_ref=where,
            send_sem=send_sem.at[k // count],
            recv_sem=ring_sem.at[k, side, letter, hop],
            device_id={"shard": shard_at(sign)},
            device_id_type=MESH,
        )

    def ring_arrival(k, side, letter, hop):
        sign = 1 - 2 * side
        owner = shard_at(-sign * (hop + 1))
        where = view(k, letter, owner)
        pltpu.make_async_copy(where, where, ring_sem.at[k, side, letter, hop]).wait()
        return owner

    def pair_copy(k, letter, owner):
        where = view(k, letter, owner)
        pltpu.make_async_remote_copy(
            src_ref=where,
            dst_ref=where,
            send_sem=send_sem.at[k // count],
            recv_sem=pair_sem.at[k // count],
            device_id={"shard": sibling},
            device_id_type=MESH,
        ).start()

    def hops(side, letter):
        return half if side == letter else half - 1

    small_writes = [
        pltpu.make_async_copy(held.at[m], small_outs[m], out_sem.at[m]) for m in range(3)
    ] + [pltpu.make_async_copy(gains, small_outs[3], out_sem.at[3])]
    merge(0)
    pl.semaphore_wait(barrier, n - 1 + width - 1)
    share(0)
    settle(0)
    finish(0)

    for j in range(steps + half + 1):
        if j < steps:
            for side in range(2):
                if hops(side, side) > 0:
                    ring_copy(j, side, side, 0).start()
        for hop in range(half):
            k = j - 1 - hop
            if 0 <= k < steps and hop + 1 < half:
                for side in range(2):
                    owner = ring_arrival(k, side, side, hop)
                    ring_copy(k, side, side, hop + 1).start()
                    pair_copy(k, side, owner)
        if j < steps:
            for side in range(2):
                if hops(side, 1 - side) > 0:
                    ring_copy(j, side, 1 - side, 0).start()
        for hop in range(half - 1):
            k = j - 1 - hop
            if 0 <= k < steps and hop + 1 < half - 1:
                for side in range(2):
                    owner = ring_arrival(k, side, 1 - side, hop)
                    ring_copy(k, side, 1 - side, hop + 1).start()
                    pair_copy(k, 1 - side, owner)
        if j < steps:
            for letter in range(2):
                pair_copy(j, letter, me)
        if j == 0:
            merge(1)
            share(1)
            for copy in norm_loads:
                copy.wait()
            gains[me, line] = norm_mem[0] + norm_mem[1]
            for step in range(1, width):
                pltpu.make_async_remote_copy(
                    src_ref=gains.at[me, line],
                    dst_ref=gains.at[me, line],
                    send_sem=norm_send.at[0],
                    recv_sem=norm_recv.at[0],
                    device_id={"width": lax.rem(line + step, width)},
                    device_id_type=MESH,
                ).start()
        if j == 1:
            merge(2)
            share(2)
            ours = gains.at[me, pl.ds(0, width - 1)]
            if width > 1:
                pltpu.make_async_copy(ours, ours, norm_recv.at[0]).wait()
            for step in range(1, n):
                pltpu.make_async_remote_copy(
                    src_ref=gains.at[me],
                    dst_ref=gains.at[me],
                    send_sem=norm_send.at[1],
                    recv_sem=norm_recv.at[1],
                    device_id={"shard": lax.rem(me + step, n)},
                    device_id_type=MESH,
                ).start()
        if j == steps - 1:
            block = gains.at[pl.ds(0, n - 1)]
            pltpu.make_async_copy(block, block, norm_recv.at[1]).wait()
            for copy in small_writes:
                copy.start()
        if j + 1 < steps:
            if (j + 1) % count == 0:
                settle((j + 1) // count)
            finish(j + 1)
        for side in range(2):
            for letter in (side, 1 - side):
                hop = hops(side, letter) - 1
                k = j - 2 - hop
                if hop >= 0 and 0 <= k < steps:
                    owner = ring_arrival(k, side, letter, hop)
                    pair_copy(k, letter, owner)

    for m in range(3):
        theirs = outs[m].at[pl.ds(0, chips)]
        pltpu.make_async_copy(theirs, theirs, pair_sem.at[m]).wait()
        sent = outs[m].at[pl.ds(0, n - 1)]
        pltpu.make_async_copy(sent, sent, send_sem.at[m]).wait()
        others = maxima.at[m, pl.ds(0, n - 1)]
        pltpu.make_async_copy(others, others, max_send.at[m]).wait()
    ours = gains.at[me, pl.ds(0, width - 1)]
    pltpu.make_async_copy(ours, ours, norm_send.at[0]).wait()
    block = gains.at[pl.ds(0, n - 1)]
    pltpu.make_async_copy(block, block, norm_send.at[1]).wait()
    for copy in small_writes:
        copy.wait()


def place_kernel(*refs):
    source, small = refs[0], refs[1:5]
    targets, finals, sem = refs[5:8], refs[8:12], refs[12]
    factors, gains, small_sem = refs[13:16], refs[16], refs[17]
    scales, serve = refs[18:21], refs[21]
    writes = [
        pltpu.make_async_copy(refs[18 + i], finals[i], small_sem.at[4 + i]) for i in range(4)
    ]
    loads = [
        pltpu.make_async_copy(small[i], refs[13 + i], small_sem.at[i]) for i in range(4)
    ]
    for copy in loads:
        copy.start()
    copies = []
    for m in range(3):
        for i in range(source.shape[1]):
            copies.append(
                pltpu.make_async_copy(source.at[m, i], targets[m].at[i], sem.at[m, i])
            )
    for copy in copies:
        copy.start()
    for copy in loads:
        copy.wait()
    for m in range(3):
        scales[m][...] = factors[m][...].reshape(scales[m].shape)
    blocks = [gains[i, k] for i in range(gains.shape[0]) for k in range(gains.shape[1])]
    line = jnp.concatenate(blocks, axis=1)
    serve[...] = line.reshape(serve.shape).astype(jnp.bfloat16)
    copies[0].wait()
    for copy in writes:
        copy.start()
    for copy in copies[1:] + writes:
        copy.wait()


def body(n, width, w_query, low_query, high_query, w_key, low_key, high_key, w_value, low_value, high_value, norm_train, norm_step):
    rows, columns = w_query.shape
    rank = low_query.shape[1]
    length = norm_train.shape[0]
    half = n // 4
    steps = 3 * chunks_of(rows)
    results = pl.pallas_call(
        functools.partial(gather_kernel, n, width),
        name="merge_gather",
        out_shape=[pltpu.VMEM((3, n, rows, columns), jnp.bfloat16)]
        + [jax.ShapeDtypeStruct((1, columns), jnp.float32)] * 3
        + [jax.ShapeDtypeStruct((n, width, 1, length), jnp.float32)],
        in_specs=[ANY] * 11,
        out_specs=[pl.BlockSpec(memory_space=pltpu.VMEM)]
        + [pl.BlockSpec(memory_space=pltpu.HBM)] * 4,
        scratch_shapes=[
            pltpu.VMEM((3, rows, columns), jnp.bfloat16),
            pltpu.VMEM((3, rows, rank), jnp.bfloat16),
            pltpu.VMEM((3, rank, columns), jnp.bfloat16),
            pltpu.VMEM((2, 1, length), jnp.float32),
            pltpu.VMEM((3, rows, columns), jnp.float32),
            pltpu.VMEM((3, 1, columns), jnp.float32),
            pltpu.VMEM((3, n, 1, columns), jnp.float32),
            pltpu.SemaphoreType.DMA((4, 3)),
            pltpu.SemaphoreType.DMA((3,)),
            pltpu.SemaphoreType.DMA((3,)),
            pltpu.SemaphoreType.DMA((3,)),
            pltpu.SemaphoreType.DMA((2,)),
            pltpu.SemaphoreType.DMA((2,)),
            pltpu.SemaphoreType.DMA((steps, 2, 2, half)),
            pltpu.SemaphoreType.DMA((3,)),
            pltpu.VMEM((3, rank, rows), jnp.bfloat16),
            pltpu.VMEM((3, 1, columns), jnp.float32),
            pltpu.VMEM((n, width, 1, length), jnp.float32),
            pltpu.SemaphoreType.DMA((4,)),
        ],
        compiler_params=pltpu.CompilerParams(
            collective_id=0, has_side_effects=True, vmem_limit_bytes=20 * 2**20
        ),
    )(
        w_query, w_key, w_value,
        low_query.T, low_key.T, low_value.T,
        high_query, high_key, high_value,
        norm_train.reshape(1, length), norm_step.reshape(1, length),
    )
    placed = pl.pallas_call(
        place_kernel,
        name="place",
        out_shape=[jax.ShapeDtypeStruct((n, rows, columns), jnp.bfloat16)] * 3
        + [jax.ShapeDtypeStruct((columns,), jnp.float32)] * 3
        + [jax.ShapeDtypeStruct((n * width * length,), jnp.bfloat16)],
        in_specs=[ANY] + [pl.BlockSpec(memory_space=pltpu.HBM)] * 4,
        out_specs=[ANY] * 3 + [pl.BlockSpec(memory_space=pltpu.HBM)] * 4,
        scratch_shapes=[
            pltpu.SemaphoreType.DMA((3, n)),
            *[pltpu.VMEM((1, columns), jnp.float32)] * 3,
            pltpu.VMEM((n, width, 1, length), jnp.float32),
            pltpu.SemaphoreType.DMA((8,)),
            *[pltpu.VMEM((columns,), jnp.float32)] * 3,
            pltpu.VMEM((n * width * length,), jnp.bfloat16),
        ],
        compiler_params=pltpu.CompilerParams(vmem_limit_bytes=2**20),
    )(pltpu.with_memory_space_constraint(results[0], pltpu.VMEM), *(pltpu.with_memory_space_constraint(small, pltpu.HBM) for small in results[1:]))
    return (
        *(ready.reshape(n * rows, columns) for ready in placed[0:3]),
        *placed[3:],
    )


def solution(mesh):
    n, width = mesh.shape["shard"], mesh.shape["width"]
    return jax.shard_map(
        functools.partial(body, n, width),
        mesh=mesh,
        in_specs=(
            P("shard", "width"),
            P("shard", None),
            P(None, "width"),
            P("shard", "width"),
            P("shard", None),
            P(None, "width"),
            P("shard", "width"),
            P("shard", None),
            P(None, "width"),
            P(("shard", "width")),
            P(("shard", "width")),
        ),
        out_specs=(
            P(None, "width"),
            P(None, "width"),
            P(None, "width"),
            P("width"),
            P("width"),
            P("width"),
            P(),
        ),
        check_vma=False,
    )
```
